32 devices in a mesh: batch: 4 (over y, x), field: 2 (over core), dim: 4 (over z).
Axes of the slice: x: 2, y: 2, z: 4, core: 2. Of those that a mesh axis runs over, the one named last changes fastest.
Arguments:
- features: bfloat16 [26, 128, 4096], P('field', 'dim', 'batch'), may hold values from -6 to 6
- cross_weight: bfloat16 [2, 26, 128, 26, 128], P(None, 'field', 'dim'), may hold values from -0.109375 to 0.109375
- cross_bias: float32 [2, 26, 128], P(None, 'field', 'dim'), may hold values from -3 to 3
- tower_weight: bfloat16 [1024, 26, 128], P(('field', 'dim')), may hold values from -0.109375 to 0.109375
- tower_bias: float32 [1024], P(('field', 'dim')), may hold values from -3 to 3
- query_weight: bfloat16 [1024, 128], P(('field', 'dim')), may hold values from -0.1875 to 0.1875
- user_vec: bfloat16 [4096, 128], P('batch'), may hold values from -6 to 6
- candidates: bfloat16 [1024, 128], P('batch'), may hold values from -6 to 6
- positive: int32 [4096], P('batch'), may hold values from 0 to 1023
Outputs:
- crossed: bfloat16 [26, 128, 4096], P('field', 'dim', 'batch')
- losses: float32 [4096], P('batch')
The draws below stay inside these ranges and needn't reach their ends.
All inputs are finite; a program needn't handle non-finite values.
Results may differ from the reference program's by a relative error of at most 0.0049.
Values may be sent and summed in bfloat16 or wider, within the bound.
A program may use at most 64 MiB of HBM per device.

```python
import math
import jax
import jax.numpy as jnp
from jax import lax

FIELDS = 26
EMB = 128
TOWER = 1024
CROSS = 2
EX_DEV = 1024
BATCH = 4096
CANDS = 1024
N_BATCH = 4


def draw_user_vec(key, part):
    row_total = BATCH
    values = jnp.clip(jax.random.normal(jax.random.fold_in(key, 11), (row_total, EMB), jnp.float32), -6.0, 6.0)
    return values.astype(jnp.bfloat16)


def draw_candidates(key, part):
    row_total = CANDS
    values = jnp.clip(jax.random.normal(jax.random.fold_in(key, 23), (row_total, EMB), jnp.float32), -6.0, 6.0)
    return values.astype(jnp.bfloat16)


def plant(entries, rng, low, top_value):
    extent = entries.shape
    spot = [jax.random.randint(jax.random.fold_in(rng, axis), (), 0, extent[axis]) for axis in range(len(extent))]
    entries = entries.at[tuple(spot)].set(low)
    longest = extent.index(max(extent))
    spot[longest] = (spot[longest] + 1) % extent[longest]
    return entries.at[tuple(spot)].set(top_value)


def steps_of(rng, dims, split, least, largest):
    loudness = 1.0
    for dim, parts in split:
        draws = jax.random.uniform(jax.random.fold_in(jax.random.fold_in(rng, 6), dim), (parts,), jnp.float32, least / len(split), largest / len(split))
        loudness = loudness * jnp.repeat(jnp.exp(draws), dims[dim] // parts).reshape((-1,) + (1,) * (len(dims) - 1 - dim))
    return loudness


def normal_values(own_key, shape, deviation, most, cuts=(), kind=jnp.bfloat16):
    values = deviation * jax.random.normal(own_key, shape, jnp.float32)
    if cuts:
        values = values * steps_of(own_key, shape, cuts, -0.22, 0.18)
    return jnp.clip(values, -most, most).astype(kind)


def setup_inputs(seed: int = 0) -> dict:
    key_of = jax.random.split(jax.random.key(seed), 10)
    return {
        "features": normal_values(key_of[0], (FIELDS, EMB, BATCH), 1.0, 6.0, ((0, 2), (1, 4), (2, 4))),
        "cross_weight": normal_values(key_of[1], (CROSS, FIELDS, EMB, FIELDS, EMB), (FIELDS * EMB) ** -0.5, 0.109375, ((1, 2), (2, 4))),
        "cross_bias": normal_values(key_of[2], (CROSS, FIELDS, EMB), 0.5, 3.0, ((1, 2), (2, 4)), jnp.float32),
        "tower_weight": normal_values(key_of[3], (TOWER, FIELDS, EMB), (FIELDS * EMB) ** -0.5, 0.109375, ((0, 8),)),
        "tower_bias": normal_values(key_of[4], (TOWER,), 0.5, 3.0, ((0, 8),), jnp.float32),
        "query_weight": normal_values(key_of[5], (TOWER, EMB), TOWER ** -0.5, 0.1875, ((0, 8),)),
        "user_vec": draw_user_vec(jax.random.fold_in(key_of[9], 71), 0),
        "candidates": draw_candidates(jax.random.fold_in(key_of[9], 71), 0),
        "positive": plant(jax.random.randint(key_of[8], (BATCH,), 0, CANDS), jax.random.fold_in(key_of[8], 1), 0, CANDS - 1).astype(jnp.int32),
    }


def reference(features, cross_weight, cross_bias, tower_weight, tower_bias, query_weight, user_vec, candidates, positive):
    width_all = FIELDS * EMB
    anchor = features.reshape(width_all, BATCH).T
    current = anchor
    for level_idx in range(CROSS):
        matrix = cross_weight[level_idx].reshape(width_all, width_all).T
        product = jnp.dot(current, matrix, preferred_element_type=jnp.float32) + cross_bias[level_idx].reshape(width_all)
        current = (anchor.astype(jnp.float32) * product + current.astype(jnp.float32)).astype(jnp.bfloat16)
    crossed = current.T.reshape(FIELDS, EMB, BATCH)
    tower_matrix = tower_weight.reshape(TOWER, width_all).T
    hidden = jax.nn.relu(jnp.dot(current, tower_matrix, preferred_element_type=jnp.float32) + tower_bias).astype(jnp.bfloat16)
    query_vec = (jnp.dot(hidden, query_weight, preferred_element_type=jnp.float32) + user_vec.astype(jnp.float32)).astype(jnp.bfloat16)
    score_scale = 1.0 / math.sqrt(EMB)

    def block_loss(inputs):
        queries, targets = inputs
        logits = jnp.dot(queries, candidates.T, preferred_element_type=jnp.float32) * score_scale
        picked = jnp.take_along_axis(logits, targets[:, None], axis=1)[:, 0]
        return jax.nn.logsumexp(logits, axis=1) - picked
    losses = lax.map(block_loss, (query_vec.reshape(N_BATCH, EX_DEV, EMB), positive.reshape(N_BATCH, EX_DEV)))
    return (crossed, losses.reshape(BATCH))
```

```python
import functools
import math

import jax
import jax.numpy as jnp
from jax import lax
from jax.experimental import pallas as pl
from jax.experimental.pallas import tpu as pltpu
from jax.sharding import PartitionSpec as P

CROSS = 2
MESH = pl.DeviceIdType.MESH


def chunk_count(row_count, member_count):
    chunks = 4
    while chunks > 1 and (row_count % (chunks * 128) or member_count % chunks):
        chunks //= 2
    return chunks


def cross_kernel(
    field_count, dim_count, chunks, feat, weight, bias, out, rows_out,
    x0, x1, raw, flat, stage, sent, rows,
    feat_sem, weight_sem, right_sem, left_sem, pair_sem, recv_sem, pair_recv, row_send, row_recv,
):
    f = lax.axis_index("field")
    d = lax.axis_index("dim")
    me = f * dim_count + d
    members = field_count * dim_count
    fl, el, row_count = feat.shape
    columns = fl * el
    fields, width, rc = x0.shape[1:]
    share = row_count // members
    per_chunk = members // chunks
    buffers = (x0, x1)
    other = field_count - 1 - f
    to_right = jnp.minimum(d + 1, dim_count - 1)
    to_left = jnp.maximum(d - 1, 0)

    def place(ff, o):
        return pl.ds(ff * fl, fl), pl.ds(pl.multiple_of(o * el, el), el)

    def piece(buffer, c, ff, o):
        fs, ds = place(ff, o)
        return buffer.at[c, fs, ds, :]

    def right(ph, c, o):
        ref = piece(buffers[ph], c, f, o)
        return pltpu.make_async_remote_copy(
            ref, ref, right_sem.at[ph, c, o], recv_sem.at[ph, c, o],
            device_id={"dim": to_right}, device_id_type=MESH)

    def left(ph, c, o):
        ref = piece(buffers[ph], c, f, o)
        return pltpu.make_async_remote_copy(
            ref, ref, left_sem.at[ph, c, o], recv_sem.at[ph, c, o],
            device_id={"dim": to_left}, device_id_type=MESH)

    def pair(ph, c, o, ff):
        ref = piece(buffers[ph], c, ff, o)
        return pltpu.make_async_remote_copy(
            ref, ref, pair_sem.at[ph, c, o], pair_recv.at[ph, c, o],
            device_id={"field": other}, device_id_type=MESH)

    def issue_own(ph, c):
        @pl.when(d < dim_count - 1)
        def _():
            right(ph, c, d).start()

        @pl.when(d > 0)
        def _():
            left(ph, c, d).start()

        pair(ph, c, d, f).start()

    def forwards(ph, c):
        for s in range(1, dim_count):
            @pl.when(d - s >= 0)
            def _():
                right(ph, c, d - s).wait_recv()

                @pl.when(d < dim_count - 1)
                def _():
                    right(ph, c, d - s).start()

                pair(ph, c, d - s, f).start()

            @pl.when(d + s < dim_count)
            def _():
                left(ph, c, d + s).wait_recv()

                @pl.when(d > 0)
                def _():
                    left(ph, c, d + s).start()

                pair(ph, c, d + s, f).start()
        for o in range(dim_count):
            pair(ph, c, o, other).wait_recv()

    def relayout(level):
        pltpu.make_async_copy(weight.at[level], raw.at[level], weight_sem.at[level]).wait()

        def group(g, carry):
            base = pl.multiple_of(g * 16, 16)
            for i in range(16):
                stage[i * 32:i * 32 + fields, :] = raw[level, base + i].astype(jnp.float32)
            for ff in range(fields):
                flat[level, pl.ds(base, 16), ff * width:(ff + 1) * width] = stage[
                    pl.ds(ff, 16, stride=32), :].astype(jnp.bfloat16)
            return carry

        lax.fori_loop(0, columns // 16, group, 0)

    def advance(ph, c):
        whole = buffers[ph][c].reshape(fields * width, rc)
        product = jnp.dot(flat[ph], whole, preferred_element_type=jnp.float32) + bias[ph]
        fs, ds = place(f, d)
        anchor = x0[c, fs, ds, :].astype(jnp.float32).reshape(columns, rc)
        current = buffers[ph][c, fs, ds, :].astype(jnp.float32).reshape(columns, rc)
        return (anchor * product + current).astype(jnp.bfloat16).reshape(fl, el, rc)

    def row_copy(m):
        fs, ds = place(f, d)
        return pltpu.make_async_remote_copy(
            sent.at[m], rows.at[fs, ds, :], row_send.at[m], row_recv.at[me],
            device_id={"field": m // dim_count, "dim": m % dim_count}, device_id_type=MESH)

    own_copies = []
    for c in range(chunks):
        copy = pltpu.make_async_copy(
            feat.at[:, :, pl.ds(c * rc, rc)], piece(x0, c, f, d), feat_sem.at[c])
        copy.start()
        own_copies.append(copy)
    for level in range(CROSS):
        pltpu.make_async_copy(weight.at[level], raw.at[level], weight_sem.at[level]).start()

    barrier = pltpu.get_barrier_semaphore()
    for k in range(1, members):
        m = lax.rem(me + k, members)
        pl.semaphore_signal(
            barrier, inc=1, device_id={"field": m // dim_count, "dim": m % dim_count},
            device_id_type=MESH)
    pl.semaphore_wait(barrier, members - 1)
    for copy in own_copies:
        copy.wait()
    issue_own(0, 0)
    if chunks > 1:
        issue_own(0, 1)
    relayout(0)

    def first(c, carry):
        forwards(0, c)
        fs, ds = place(f, d)
        x1[c, fs, ds, :] = advance(0, c)
        issue_own(1, c)

        @pl.when(c + 2 < chunks)
        def _():
            issue_own(0, c + 2)

        return carry

    lax.fori_loop(0, chunks, first, 0)
    relayout(1)

    def second(c, carry):
        forwards(1, c)
        new = advance(1, c)
        out[:, :, pl.ds(pl.multiple_of(c * rc, 128), rc)] = new
        for j in range(per_chunk):
            m = c * per_chunk + j
            part = new[:, :, j * share:(j + 1) * share]

            @pl.when(m == me)
            def _():
                fs, ds = place(f, d)
                rows[fs, ds, :] = part

            @pl.when(m != me)
            def _():
                sent[m] = part
                row_copy(m).start()

        return carry

    lax.fori_loop(0, chunks, second, 0)

    for k in range(1, members):
        m = lax.rem(me + k, members)
        fs, ds = place(m // dim_count, m % dim_count)
        ref = rows.at[fs, ds, :]
        pltpu.make_async_remote_copy(
            sent.at[m], ref, row_send.at[m], row_recv.at[m],
            device_id={"field": m // dim_count, "dim": m % dim_count}, device_id_type=MESH,
        ).wait_recv()
        row_copy(m).wait_send()
    rows_out[...] = rows[...]

    def drain(c, carry):
        for ph in range(CROSS):
            for o in range(dim_count):
                @pl.when((o <= d) & (d < dim_count - 1))
                def _():
                    right(ph, c, o).wait_send()

                @pl.when((o >= d) & (d > 0))
                def _():
                    left(ph, c, o).wait_send()

                pair(ph, c, o, f).wait_send()
        return carry

    lax.fori_loop(0, chunks, drain, 0)


def cross_layers(features, cross_weight, cross_bias):
    field_count = lax.axis_size("field")
    dim_count = lax.axis_size("dim")
    members = field_count * dim_count
    fl, el, row_count = features.shape
    columns = fl * el
    fields, width = cross_weight.shape[3:]
    chunks = chunk_count(row_count, members)
    rc = row_count // chunks
    share = row_count // members
    steps = (CROSS, chunks, dim_count)
    dma = pltpu.SemaphoreType.DMA
    return pl.pallas_call(
        functools.partial(cross_kernel, field_count, dim_count, chunks),
        out_shape=(
            jax.ShapeDtypeStruct(features.shape, jnp.bfloat16),
            jax.ShapeDtypeStruct((fields, width, share), jnp.bfloat16),
        ),
        in_specs=[
            pl.BlockSpec(memory_space=pl.ANY),
            pl.BlockSpec(memory_space=pl.ANY),
            pl.BlockSpec(memory_space=pltpu.VMEM),
        ],
        out_specs=(
            pl.BlockSpec(memory_space=pltpu.VMEM),
            pl.BlockSpec(memory_space=pltpu.VMEM),
        ),
        scratch_shapes=[
            pltpu.VMEM((chunks, fields, width, rc), jnp.bfloat16),
            pltpu.VMEM((chunks, fields, width, rc), jnp.bfloat16),
            pltpu.VMEM((CROSS, columns, fields, width), jnp.bfloat16),
            pltpu.VMEM((CROSS, columns, fields * width), jnp.bfloat16),
            pltpu.VMEM((16 * 32, width), jnp.float32),
            pltpu.VMEM((members, fl, el, share), jnp.bfloat16),
            pltpu.VMEM((fields, width, share), jnp.bfloat16),
            dma((chunks,)),
            dma((CROSS,)),
            dma(steps),
            dma(steps),
            dma(steps),
            dma(steps),
            dma(steps),
            dma((members,)),
            dma((members,)),
        ],
        compiler_params=pltpu.CompilerParams(
            collective_id=0, has_side_effects=True, vmem_limit_bytes=52 * 2**20),
        cost_estimate=pl.CostEstimate(
            flops=4 * columns * fields * width * row_count,
            bytes_accessed=400_000_000, transcendentals=0),
        name="cross_layers",
    )(
        features,
        cross_weight.reshape(CROSS, columns, fields, width),
        cross_bias.reshape(CROSS, columns, 1),
    )


def spread(block):
    units = block.shape[0]
    batch_count = lax.axis_size("batch")
    split = batch_count if units % (batch_count * 16) == 0 else 1
    if split == 1:
        return lax.all_gather(block, ("field", "dim"), axis=0, tiled=True), split
    part = units // split
    mine = lax.dynamic_slice_in_dim(block, lax.axis_index("batch") * part, part, 0)
    level = lax.all_gather(mine, ("field", "dim"), axis=0, tiled=True)
    return lax.all_gather(level, "batch", axis=0, tiled=True), split


def regroup(whole, members, split):
    shaped = whole.reshape((members, split, -1) + whole.shape[1:])
    return jnp.swapaxes(shaped, 0, 1).reshape(whole.shape)


def body(
    features, cross_weight, cross_bias, tower_weight, tower_bias, query_weight,
    user_vec, candidates, positive,
):
    members = lax.axis_size("field") * lax.axis_size("dim")
    row_count = features.shape[2]
    fields, width = tower_weight.shape[1:]
    tower_all, split = spread(tower_weight.reshape(-1, fields * width))
    query_all = lax.all_gather(query_weight, ("field", "dim"), axis=0, tiled=True)
    bias_all = lax.all_gather(tower_bias, ("field", "dim"), axis=0, tiled=True)
    query_all = regroup(query_all, members, split)
    bias_all = regroup(bias_all, members, split)
    candidates_all = lax.all_gather(candidates, "batch", axis=0, tiled=True)
    crossed, rows = cross_layers(features, cross_weight, cross_bias)
    share = row_count // members
    start = lax.axis_index(("field", "dim")) * share
    tower_pre = jnp.dot(
        tower_all, rows.reshape(fields * width, share), preferred_element_type=jnp.float32)
    hidden = jax.nn.relu(tower_pre + bias_all[:, None]).astype(jnp.bfloat16)
    query = lax.dot_general(
        hidden, query_all, (((0,), (0,)), ((), ())), preferred_element_type=jnp.float32)
    user_rows = lax.dynamic_slice_in_dim(user_vec, start, share, 0)
    targets = lax.dynamic_slice_in_dim(positive, start, share, 0)
    query_vec = (query + user_rows.astype(jnp.float32)).astype(jnp.bfloat16)
    logits = lax.dot_general(
        query_vec, candidates_all, (((1,), (1,)), ((), ())), preferred_element_type=jnp.float32
    ) * (1.0 / math.sqrt(query_vec.shape[1]))
    labels = lax.broadcasted_iota(jnp.int32, logits.shape, 1)
    picked = jnp.sum(jnp.where(labels == targets[:, None], logits, 0.0), axis=1)
    best = jnp.max(logits, axis=1)
    total = jnp.sum(jnp.exp(logits - best[:, None]), axis=1)
    part_loss = best + jnp.log(total) - picked
    losses = lax.all_gather(part_loss, ("field", "dim"), axis=0, tiled=True)
    return (crossed, losses)


def solution(mesh):
    placed = (
        P("field", "dim", "batch"),
        P(None, "field", "dim", None, None),
        P(None, "field", "dim"),
        P(("field", "dim"), None, None),
        P(("field", "dim")),
        P(("field", "dim"), None),
        P("batch", None),
        P("batch", None),
        P("batch"),
    )
    return jax.shard_map(
        body,
        mesh=mesh,
        in_specs=placed,
        out_specs=(P("field", "dim", "batch"), P("batch")),
        check_vma=False,
    )
```

```python
import functools
import math

import jax
import jax.numpy as jnp
from jax import lax
from jax.experimental import pallas as pl
from jax.experimental.pallas import tpu as pltpu
from jax.sharding import PartitionSpec as P

CROSS = 2
MESH = pl.DeviceIdType.MESH


def chunk_count(row_count, member_count):
    chunks = 4
    while chunks > 1 and (row_count % (chunks * 128) or member_count % chunks):
        chunks //= 2
    return chunks


def rank_kernel(
    counts, splits,
    feat, weight, bias, tower, tower_bias, query_weight, user, cand, positive,
    out, loss_out,
    x0, x1, flat, sent, rows, towers, biases, columns_bias, queries, cands, losses,
    feat_sem, weight_sem, tower_sem, small_sem,
    right_sem, left_sem, pair_sem, recv_sem, pair_recv,
    row_send, row_recv, chain_right, chain_left, chain_recv, both_send, both_recv,
    plane_send, plane_recv, plane_pair, plane_pair_recv,
    cand_send, cand_recv, loss_send, loss_recv,
):
    batch_count, field_count, dim_count = counts
    chunks, split = splits
    b = lax.axis_index("batch")
    f = lax.axis_index("field")
    d = lax.axis_index("dim")
    me = f * dim_count + d
    members = field_count * dim_count
    fl, el, row_count = feat.shape
    columns = fl * el
    fields, width, rc = x0.shape[1:]
    share = row_count // members
    per_chunk = members // chunks
    part = towers.shape[2]
    units = split * part
    buffers = (x0, x1)
    other = field_count - 1 - f
    mine = b if split > 1 else 0
    to_right = jnp.minimum(d + 1, dim_count - 1)
    to_left = jnp.maximum(d - 1, 0)

    def remote(ref, send, recv, **where):
        return pltpu.make_async_remote_copy(
            ref, ref, send, recv, device_id=where, device_id_type=MESH)

    def place(ff, o):
        return pl.ds(ff * fl, fl), pl.ds(pl.multiple_of(o * el, el), el)

    def piece(ph, c, ff, o):
        fs, ds = place(ff, o)
        return buffers[ph].at[c, fs, ds, :]

    def right(ph, c, o):
        return remote(piece(ph, c, f, o), right_sem.at[ph, c, o], recv_sem.at[ph, c, o], dim=to_right)

    def left(ph, c, o):
        return remote(piece(ph, c, f, o), left_sem.at[ph, c, o], recv_sem.at[ph, c, o], dim=to_left)

    def pair(ph, c, o, ff):
        return remote(
            piece(ph, c, ff, o), pair_sem.at[ph, c, o], pair_recv.at[ph, c, o], field=other)

    def issue_own(ph, c):
        @pl.when(d < dim_count - 1)
        def _():
            right(ph, c, d).start()

        @pl.when(d > 0)
        def _():
            left(ph, c, d).start()

        pair(ph, c, d, f).start()

    def forwards(ph, c):
        for s in range(1, dim_count):
            @pl.when(d - s >= 0)
            def _():
                right(ph, c, d - s).wait_recv()

                @pl.when(d < dim_count - 1)
                def _():
                    right(ph, c, d - s).start()

                pair(ph, c, d - s, f).start()

            @pl.when(d + s < dim_count)
            def _():
                left(ph, c, d + s).wait_recv()

                @pl.when(d > 0)
                def _():
                    left(ph, c, d + s).start()

                pair(ph, c, d + s, f).start()
        for o in range(dim_count):
            pair(ph, c, o, other).wait_recv()

    def weight_copy(level, ff):
        return pltpu.make_async_copy(
            weight.at[level, :, ff],
            flat.at[level, :, :, pl.ds(pl.multiple_of(ff * width, width), width)],
            weight_sem.at[level, ff])

    def tower_copy(ff):
        return pltpu.make_async_copy(
            tower.at[ff, pl.ds(pl.multiple_of(mine * part, part), part), :],
            towers.at[mine, me, :, pl.ds(pl.multiple_of(ff * width, width), width)],
            tower_sem.at[ff])

    def each_field(act):
        def step(ff, carry):
            act(ff)
            return carry

        lax.fori_loop(0, fields, step, 0)

    small_refs = (
        lambda o: towers.at[mine, f * dim_count + o],
        lambda o: queries.at[:, f * dim_count + o],
        lambda o: biases.at[f * dim_count + o],
    )
    small_wide = (
        lambda ff: towers.at[mine, pl.ds(ff * dim_count, dim_count)],
        lambda ff: queries.at[:, pl.ds(ff * dim_count, dim_count)],
        lambda ff: biases.at[pl.ds(ff * dim_count, dim_count)],
    )

    def chain_to(k, o, sems, target):
        return remote(small_refs[k](o), sems.at[k, o], chain_recv.at[k, o], dim=target)

    def chain_own():
        for k in range(3):
            @pl.when(d < dim_count - 1)
            def _():
                chain_to(k, d, chain_right, to_right).start()

            @pl.when(d > 0)
            def _():
                chain_to(k, d, chain_left, to_left).start()

    def chain_step(s):
        for k in range(3):
            @pl.when(d - s >= 0)
            def _():
                chain_to(k, d - s, chain_right, to_right).wait_recv()

                @pl.when(d < dim_count - 1)
                def _():
                    chain_to(k, d - s, chain_right, to_right).start()

            @pl.when(d + s < dim_count)
            def _():
                chain_to(k, d + s, chain_left, to_left).wait_recv()

                @pl.when(d > 0)
                def _():
                    chain_to(k, d + s, chain_left, to_left).start()

    def both(k, ff):
        return remote(small_wide[k](ff), both_send.at[k], both_recv.at[k], field=other)

    def plane(t, source):
        return remote(
            towers.at[source, pl.ds(f * dim_count, dim_count)],
            plane_send.at[t], plane_recv.at[source], batch=t)

    def plane_both(source, ff):
        return remote(
            towers.at[source, pl.ds(ff * dim_count, dim_count)],
            plane_pair.at[source], plane_pair_recv.at[source], field=other)

    def cand_copy(t, source):
        return remote(cands.at[source], cand_send.at[t], cand_recv.at[source], batch=t)

    def loss_copy(m, source):
        return remote(
            losses.at[source], loss_send.at[m], loss_recv.at[source],
            field=m // dim_count, dim=m % dim_count)

    def row_copy(m):
        fs, ds = place(f, d)
        return pltpu.make_async_remote_copy(
            sent.at[m], rows.at[fs, ds, :], row_send.at[m], row_recv.at[me],
            device_id={"field": m // dim_count, "dim": m % dim_count}, device_id_type=MESH)

    def advance(ph, c):
        whole = buffers[ph][c].reshape(fields * width, rc)
        matrix = flat[ph].reshape(columns, fields * width)
        product = jnp.dot(matrix, whole, preferred_element_type=jnp.float32) + bias[ph]
        fs, ds = place(f, d)
        anchor = x0[c, fs, ds, :].astype(jnp.float32).reshape(columns, rc)
        current = buffers[ph][c, fs, ds, :].astype(jnp.float32).reshape(columns, rc)
        return (anchor * product + current).astype(jnp.bfloat16).reshape(fl, el, rc)

    own_copies = []
    for c in range(chunks):
        own_copies.append(pltpu.make_async_copy(
            feat.at[:, :, pl.ds(c * rc, rc)], piece(0, c, f, d), feat_sem.at[c]))
    small_copies = [
        pltpu.make_async_copy(query_weight, queries.at[:, me], small_sem.at[0]),
        pltpu.make_async_copy(tower_bias, biases.at[me], small_sem.at[1]),
        pltpu.make_async_copy(cand, cands.at[b], small_sem.at[2]),
    ]
    for copy in own_copies + small_copies:
        copy.start()
    each_field(lambda ff: tower_copy(ff).start())
    for level in range(CROSS):
        each_field(lambda ff: weight_copy(level, ff).start())

    barrier = pltpu.get_barrier_semaphore()
    for k in range(1, members):
        m = lax.rem(me + k, members)
        pl.semaphore_signal(
            barrier, inc=1, device_id={"field": m // dim_count, "dim": m % dim_count},
            device_id_type=MESH)
    for k in range(1, batch_count):
        pl.semaphore_signal(
            barrier, inc=1, device_id={"batch": lax.rem(b + k, batch_count)}, device_id_type=MESH)
    pl.semaphore_wait(barrier, members + batch_count - 2)
    for copy in own_copies:
        copy.wait()
    issue_own(0, 0)
    if chunks > 1:
        issue_own(0, 1)
    each_field(lambda ff: tower_copy(ff).wait())
    for copy in small_copies:
        copy.wait()
    chain_own()
    for k in range(1, batch_count):
        cand_copy(lax.rem(b + k, batch_count), b).start()
    for level in range(CROSS):
        each_field(lambda ff: weight_copy(level, ff).wait())

    def first(c, carry):
        forwards(0, c)
        fs, ds = place(f, d)
        x1[c, fs, ds, :] = advance(0, c)
        issue_own(1, c)

        @pl.when(c + 2 < chunks)
        def _():
            issue_own(0, c + 2)

        for s in range(1, min(chunks, dim_count)):
            @pl.when(c == s)
            def _():
                chain_step(s)

        return carry

    lax.fori_loop(0, chunks, first, 0)
    for s in range(min(chunks, dim_count), dim_count):
        chain_step(s)
    for k in range(3):
        both(k, f).start()
    if split > 1:
        for k in range(1, split):
            plane(lax.rem(b + k, split), b).start()

    def second(c, carry):
        forwards(1, c)
        new = advance(1, c)
        out[:, :, pl.ds(pl.multiple_of(c * rc, 128), rc)] = new
        for j in range(per_chunk):
            m = c * per_chunk + j
            piece_rows = new[:, :, j * share:(j + 1) * share]

            @pl.when(m == me)
            def _():
                fs, ds = place(f, d)
                rows[fs, ds, :] = piece_rows

            @pl.when(m != me)
            def _():
                sent[m] = piece_rows
                row_copy(m).start()

        return carry

    lax.fori_loop(0, chunks, second, 0)

    if split > 1:
        for k in range(1, split):
            source = lax.rem(b + k, split)
            plane(source, source).wait_recv()
            plane_both(source, f).start()
    for k in range(3):
        both(k, other).wait_recv()
    for k in range(1, batch_count):
        source = lax.rem(b + k, batch_count)
        cand_copy(source, source).wait_recv()
    for m in range(members):
        block = jnp.broadcast_to(biases[m], (share, units)).T
        columns_bias[:, m] = block.reshape(split, part, share)
    if split > 1:
        for k in range(1, split):
            plane_both(lax.rem(b + k, split), other).wait_recv()
    for k in range(1, members):
        m = lax.rem(me + k, members)
        fs, ds = place(m // dim_count, m % dim_count)
        remote(rows.at[fs, ds, :], row_send.at[m], row_recv.at[m],
               field=m // dim_count, dim=m % dim_count).wait_recv()

    def tower_block(s, query):
        matrix = towers[s].reshape(members * part, fields * width)
        pre = jnp.dot(
            matrix, rows[...].reshape(fields * width, share), preferred_element_type=jnp.float32)
        pre = pre + columns_bias[s].reshape(members * part, share)
        hidden = jnp.maximum(pre, 0.0).astype(jnp.bfloat16)
        return query + lax.dot_general(
            hidden, queries[s].reshape(members * part, width), (((0,), (0,)), ((), ())),
            preferred_element_type=jnp.float32)

    query = lax.fori_loop(0, split, tower_block, jnp.zeros((share, width), jnp.float32))
    start = pl.multiple_of(me * share, share)
    query_vec = (query + user[pl.ds(start, share), :].astype(jnp.float32)).astype(jnp.bfloat16)
    all_cands = cands[...].reshape(-1, width)
    logits = lax.dot_general(
        all_cands, query_vec, (((1,), (1,)), ((), ())), preferred_element_type=jnp.float32
    ) * (1.0 / math.sqrt(width))
    labels = lax.broadcasted_iota(jnp.int32, logits.shape, 0)
    picked = jnp.sum(jnp.where(labels == positive[me], logits, 0.0), axis=0, keepdims=True)
    best = jnp.max(logits, axis=0, keepdims=True)
    total = jnp.sum(jnp.exp(logits - best), axis=0, keepdims=True)
    losses[me] = best + jnp.log(total) - picked
    for k in range(1, members):
        loss_copy(lax.rem(me + k, members), me).start()

    def drain(c, carry):
        for ph in range(CROSS):
            for o in range(dim_count):
                @pl.when((o <= d) & (d < dim_count - 1))
                def _():
                    right(ph, c, o).wait_send()

                @pl.when((o >= d) & (d > 0))
                def _():
                    left(ph, c, o).wait_send()

                pair(ph, c, o, f).wait_send()
        return carry

    lax.fori_loop(0, chunks, drain, 0)
    for k in range(3):
        for o in range(dim_count):
            @pl.when((o <= d) & (d < dim_count - 1))
            def _():
                chain_to(k, o, chain_right, to_right).wait_send()

            @pl.when((o >= d) & (d > 0))
            def _():
                chain_to(k, o, chain_left, to_left).wait_send()

        both(k, f).wait_send()
    if split > 1:
        for k in range(1, split):
            t = lax.rem(b + k, split)
            plane(t, b).wait_send()
            plane_both(t, f).wait_send()
    for k in range(1, batch_count):
        cand_copy(lax.rem(b + k, batch_count), b).wait_send()
    for k in range(1, members):
        m = lax.rem(me + k, members)
        row_copy(m).wait_send()
        loss_copy(m, m).wait_recv()
        loss_copy(m, me).wait_send()
    loss_out[...] = losses[...]


def body(
    features, cross_weight, cross_bias, tower_weight, tower_bias, query_weight,
    user_vec, candidates, positive,
):
    counts = tuple(lax.axis_size(name) for name in ("batch", "field", "dim"))
    batch_count, field_count, dim_count = counts
    members = field_count * dim_count
    fl, el, row_count = features.shape
    columns = fl * el
    units, fields, width = tower_weight.shape
    chunks = chunk_count(row_count, members)
    split = batch_count if units % (batch_count * 16) == 0 else 1
    part = units // split
    rc = row_count // chunks
    share = row_count // members
    steps = (CROSS, chunks, dim_count)
    small = (3, dim_count)
    dma = pltpu.SemaphoreType.DMA
    vmem = pltpu.VMEM
    bf16 = jnp.bfloat16
    far = pl.BlockSpec(memory_space=pl.ANY)
    near = pl.BlockSpec(memory_space=pltpu.VMEM)
    crossed, losses = pl.pallas_call(
        functools.partial(rank_kernel, counts, (chunks, split)),
        out_shape=(
            jax.ShapeDtypeStruct(features.shape, bf16),
            jax.ShapeDtypeStruct((members, 1, share), jnp.float32),
        ),
        in_specs=[far, far, near, far, far, far, near, far, near],
        out_specs=(near, near),
        scratch_shapes=[
            vmem((chunks, fields, width, rc), bf16),
            vmem((chunks, fields, width, rc), bf16),
            vmem((CROSS, fl, el, fields * width), bf16),
            vmem((members, fl, el, share), bf16),
            vmem((fields, width, share), bf16),
            vmem((split, members, part, fields * width), bf16),
            vmem((members, 1, units), jnp.float32),
            vmem((split, members, part, share), jnp.float32),
            vmem((split, members, part, width), bf16),
            vmem((batch_count,) + candidates.shape, bf16),
            vmem((members, 1, share), jnp.float32),
            dma((chunks,)), dma((CROSS, fields)), dma((fields,)), dma((3,)),
            dma(steps), dma(steps), dma(steps), dma(steps), dma(steps),
            dma((members,)), dma((members,)), dma(small), dma(small), dma(small),
            dma((3,)), dma((3,)),
            dma((split,)), dma((split,)), dma((split,)), dma((split,)),
            dma((batch_count,)), dma((batch_count,)), dma((members,)), dma((members,)),
        ],
        compiler_params=pltpu.CompilerParams(
            collective_id=0, has_side_effects=True, vmem_limit_bytes=56 * 2**20),
        name="rank_forward",
    )(
        features,
        cross_weight.transpose(0, 1, 3, 2, 4),
        cross_bias.reshape(CROSS, columns, 1),
        tower_weight.transpose(1, 0, 2),
        tower_bias.reshape(1, units),
        query_weight.reshape(split, part, width),
        user_vec,
        candidates,
        positive.reshape(members, 1, share),
    )
    return (crossed, losses.reshape(row_count))


def solution(mesh):
    placed = (
        P("field", "dim", "batch"),
        P(None, "field", "dim", None, None),
        P(None, "field", "dim"),
        P(("field", "dim"), None, None),
        P(("field", "dim")),
        P(("field", "dim"), None),
        P("batch", None),
        P("batch", None),
        P("batch"),
    )
    return jax.shard_map(
        body,
        mesh=mesh,
        in_specs=placed,
        out_specs=(P("field", "dim", "batch"), P("batch")),
        check_vma=False,
    )
```

```python
import functools
import math

import jax
import jax.numpy as jnp
from jax import lax
from jax.experimental import pallas as pl
from jax.experimental.pallas import tpu as pltpu
from jax.sharding import PartitionSpec as P

CROSS = 2
MESH = pl.DeviceIdType.MESH


def tower_levels(dim_count):
    held = min(2, dim_count)
    return (dim_count - held) // 2, held


def chunk_count(row_count, field_count, held):
    chunks = 4
    while chunks > field_count and row_count % (chunks * held * 128):
        chunks //= 2
    return chunks


def rank_kernel(
    counts, splits,
    feat, weight, bias, tower, tower_bias, query_weight, user, cand, positive,
    out, loss_out,
    x0, x1, flat, sent, rows, towers, biases, columns_bias, queries, cands, losses,
    feat_sem, weight_sem, tower_sem, small_sem,
    right_sem, left_sem, pair_sem, recv_sem, pair_recv,
    row_send, row_recv, chain_right, chain_left, chain_recv, both_send, both_recv,
    plane_send, plane_recv, plane_pair, plane_pair_recv,
    cand_send, cand_recv, loss_send, loss_recv,
):
    batch_count, field_count, dim_count = counts
    chunks, split = splits
    b = lax.axis_index("batch")
    f = lax.axis_index("field")
    d = lax.axis_index("dim")
    me = f * dim_count + d
    members = field_count * dim_count
    fl, el, row_count = feat.shape
    columns = fl * el
    fields, width, rc = x0.shape[1:]
    low, held = tower_levels(dim_count)
    high = low + held - 1
    level_of = d - low
    active = (d >= low) & (d <= high)
    sub = rc // held
    run = chunks // field_count
    share = run * sub
    part = towers.shape[2]
    units = split * part
    buffers = (x0, x1)
    other = field_count - 1 - f
    mine = b if split > 1 else 0
    to_right = jnp.minimum(d + 1, dim_count - 1)
    to_left = jnp.maximum(d - 1, 0)

    def remote(ref, send, recv, **where):
        return pltpu.make_async_remote_copy(
            ref, ref, send, recv, device_id=where, device_id_type=MESH)

    def place(ff, o):
        return pl.ds(ff * fl, fl), pl.ds(pl.multiple_of(o * el, el), el)

    def piece(ph, c, ff, o):
        fs, ds = place(ff, o)
        return buffers[ph].at[c, fs, ds, :]

    def right(ph, c, o):
        return remote(piece(ph, c, f, o), right_sem.at[ph, c, o], recv_sem.at[ph, c, o], dim=to_right)

    def left(ph, c, o):
        return remote(piece(ph, c, f, o), left_sem.at[ph, c, o], recv_sem.at[ph, c, o], dim=to_left)

    def pair(ph, c, o, ff):
        return remote(
            piece(ph, c, ff, o), pair_sem.at[ph, c, o], pair_recv.at[ph, c, o], field=other)

    def issue_own(ph, c):
        @pl.when(d < dim_count - 1)
        def _():
            right(ph, c, d).start()

        @pl.when(d > 0)
        def _():
            left(ph, c, d).start()

        pair(ph, c, d, f).start()

    def forwards(ph, c):
        for s in range(1, dim_count):
            @pl.when(d - s >= 0)
            def _():
                right(ph, c, d - s).wait_recv()

                @pl.when(d < dim_count - 1)
                def _():
                    right(ph, c, d - s).start()

                pair(ph, c, d - s, f).start()

            @pl.when(d + s < dim_count)
            def _():
                left(ph, c, d + s).wait_recv()

                @pl.when(d > 0)
                def _():
                    left(ph, c, d + s).start()

                pair(ph, c, d + s, f).start()
        for o in range(dim_count):
            pair(ph, c, o, other).wait_recv()

    def weight_copy(level, ff):
        return pltpu.make_async_copy(
            weight.at[level, :, ff],
            flat.at[level, :, :, pl.ds(pl.multiple_of(ff * width, width), width)],
            weight_sem.at[level, ff])

    def tower_copy(ff):
        return pltpu.make_async_copy(
            tower.at[ff, pl.ds(pl.multiple_of(mine * part, part), part), :],
            towers.at[mine, me, :, pl.ds(pl.multiple_of(ff * width, width), width)],
            tower_sem.at[ff])

    def each_field(act):
        def step(ff, carry):
            act(ff)
            return carry

        lax.fori_loop(0, fields, step, 0)

    small_refs = (
        lambda o: towers.at[mine, f * dim_count + o],
        lambda o: queries.at[:, f * dim_count + o],
        lambda o: biases.at[f * dim_count + o],
    )
    small_wide = (
        lambda ff: towers.at[mine, pl.ds(ff * dim_count, dim_count)],
        lambda ff: queries.at[:, pl.ds(ff * dim_count, dim_count)],
        lambda ff: biases.at[pl.ds(ff * dim_count, dim_count)],
    )

    def chain_to(k, o, sems, target):
        return remote(small_refs[k](o), sems.at[k, o], chain_recv.at[k, o], dim=target)

    def chain_own():
        for k in range(3):
            @pl.when(d < high)
            def _():
                chain_to(k, d, chain_right, to_right).start()

            @pl.when(d > low)
            def _():
                chain_to(k, d, chain_left, to_left).start()

    def chain_step(s):
        for k in range(3):
            @pl.when((d - s >= 0) & (d <= high))
            def _():
                chain_to(k, d - s, chain_right, to_right).wait_recv()

                @pl.when(d < high)
                def _():
                    chain_to(k, d - s, chain_right, to_right).start()

            @pl.when((d + s < dim_count) & (d >= low))
            def _():
                chain_to(k, d + s, chain_left, to_left).wait_recv()

                @pl.when(d > low)
                def _():
                    chain_to(k, d + s, chain_left, to_left).start()

    def both(k, ff):
        return remote(small_wide[k](ff), both_send.at[k], both_recv.at[k], field=other)

    def plane(t, source):
        return remote(
            towers.at[source, pl.ds(f * dim_count, dim_count)],
            plane_send.at[t], plane_recv.at[source], batch=t)

    def plane_both(source, ff):
        return remote(
            towers.at[source, pl.ds(ff * dim_count, dim_count)],
            plane_pair.at[source], plane_pair_recv.at[source], field=other)

    def cand_copy(t, source):
        return remote(cands.at[source], cand_send.at[t], cand_recv.at[source], batch=t)

    def loss_copy(m, ff, level):
        ref = losses.at[level, pl.ds(ff * run, run)]
        return remote(
            ref, loss_send.at[m], loss_recv.at[ff, level], field=m // dim_count, dim=m % dim_count)

    def row_copy(c, level):
        fs, ds = place(f, d)
        return pltpu.make_async_remote_copy(
            sent.at[c, level],
            rows.at[fs, ds, pl.ds(pl.multiple_of(lax.rem(c, run) * sub, sub), sub)],
            row_send.at[c, level], row_recv.at[lax.rem(c, run), me],
            device_id={"field": c // run, "dim": low + level}, device_id_type=MESH)

    def own_rows(c, level):
        return (c // run == f) & (level_of == level)

    def advance(ph, c):
        whole = buffers[ph][c].reshape(fields * width, rc)
        matrix = flat[ph].reshape(columns, fields * width)
        product = jnp.dot(matrix, whole, preferred_element_type=jnp.float32) + bias[ph]
        fs, ds = place(f, d)
        anchor = x0[c, fs, ds, :].astype(jnp.float32).reshape(columns, rc)
        current = buffers[ph][c, fs, ds, :].astype(jnp.float32).reshape(columns, rc)
        return (anchor * product + current).astype(jnp.bfloat16).reshape(fl, el, rc)

    own_copies = []
    for c in range(chunks):
        own_copies.append(pltpu.make_async_copy(
            feat.at[:, :, pl.ds(c * rc, rc)], piece(0, c, f, d), feat_sem.at[c]))
    small_copies = [
        pltpu.make_async_copy(query_weight, queries.at[:, me], small_sem.at[0]),
        pltpu.make_async_copy(tower_bias, biases.at[me], small_sem.at[1]),
        pltpu.make_async_copy(cand, cands.at[b], small_sem.at[2]),
    ]
    for copy in own_copies + small_copies:
        copy.start()
    each_field(lambda ff: tower_copy(ff).start())
    for level in range(CROSS):
        each_field(lambda ff: weight_copy(level, ff).start())

    barrier = pltpu.get_barrier_semaphore()
    for k in range(1, members):
        m = lax.rem(me + k, members)
        pl.semaphore_signal(
            barrier, inc=1, device_id={"field": m // dim_count, "dim": m % dim_count},
            device_id_type=MESH)
    for k in range(1, batch_count):
        pl.semaphore_signal(
            barrier, inc=1, device_id={"batch": lax.rem(b + k, batch_count)}, device_id_type=MESH)
    pl.semaphore_wait(barrier, members + batch_count - 2)
    for copy in own_copies:
        copy.wait()
    issue_own(0, 0)
    if chunks > 1:
        issue_own(0, 1)
    each_field(lambda ff: tower_copy(ff).wait())
    for copy in small_copies:
        copy.wait()
    chain_own()

    @pl.when(active)
    def _():
        for k in range(1, batch_count):
            cand_copy(lax.rem(b + k, batch_count), b).start()

    for level in range(CROSS):
        each_field(lambda ff: weight_copy(level, ff).wait())

    def first(c, carry):
        forwards(0, c)
        fs, ds = place(f, d)
        x1[c, fs, ds, :] = advance(0, c)
        issue_own(1, c)

        @pl.when(c + 2 < chunks)
        def _():
            issue_own(0, c + 2)

        for s in range(1, min(chunks, dim_count)):
            @pl.when(c == s)
            def _():
                chain_step(s)

        return carry

    lax.fori_loop(0, chunks, first, 0)
    for s in range(min(chunks, dim_count), dim_count):
        chain_step(s)

    @pl.when(active)
    def _():
        for k in range(3):
            both(k, f).start()
        if split > 1:
            for k in range(1, split):
                plane(lax.rem(b + k, split), b).start()

    def second(c, carry):
        forwards(1, c)
        new = advance(1, c)
        out[:, :, pl.ds(pl.multiple_of(c * rc, 128), rc)] = new
        for level in range(held):
            block = new[:, :, level * sub:(level + 1) * sub]

            @pl.when(own_rows(c, level))
            def _():
                fs, ds = place(f, d)
                rows[fs, ds, pl.ds(pl.multiple_of(lax.rem(c, run) * sub, sub), sub)] = block

            @pl.when(jnp.logical_not(own_rows(c, level)))
            def _():
                sent[c, level] = block
                row_copy(c, level).start()

        return carry

    lax.fori_loop(0, chunks, second, 0)

    def tower_block(s, query):
        matrix = towers[s].reshape(members * part, fields * width)
        pre = jnp.dot(
            matrix, rows[...].reshape(fields * width, share), preferred_element_type=jnp.float32)
        pre = pre + columns_bias[s].reshape(members * part, share)
        hidden = jnp.maximum(pre, 0.0).astype(jnp.bfloat16)
        return query + lax.dot_general(
            hidden, queries[s].reshape(members * part, width), (((0,), (0,)), ((), ())),
            preferred_element_type=jnp.float32)

    @pl.when(active)
    def _():
        if split > 1:
            for k in range(1, split):
                source = lax.rem(b + k, split)
                plane(source, source).wait_recv()
                plane_both(source, f).start()
        for k in range(3):
            both(k, other).wait_recv()
        for k in range(1, batch_count):
            source = lax.rem(b + k, batch_count)
            cand_copy(source, source).wait_recv()
        for m in range(members):
            block = jnp.broadcast_to(biases[m], (share, units)).T
            columns_bias[:, m] = block.reshape(split, part, share)
        if split > 1:
            for k in range(1, split):
                plane_both(lax.rem(b + k, split), other).wait_recv()
        for j in range(run):
            for k in range(1, members):
                m = lax.rem(me + k, members)
                fs, ds = place(m // dim_count, m % dim_count)
                remote(rows.at[fs, ds, pl.ds(j * sub, sub)], row_send.at[0, 0], row_recv.at[j, m],
                       field=m // dim_count, dim=m % dim_count).wait_recv()

        query = lax.fori_loop(0, split, tower_block, jnp.zeros((share, width), jnp.float32))
        all_cands = cands[...].reshape(-1, width)
        for j in range(run):
            c = f * run + j
            start = pl.multiple_of(c * rc + level_of * sub, sub)
            query_vec = (
                query[j * sub:(j + 1) * sub] + user[pl.ds(start, sub), :].astype(jnp.float32)
            ).astype(jnp.bfloat16)
            logits = lax.dot_general(
                all_cands, query_vec, (((1,), (1,)), ((), ())), preferred_element_type=jnp.float32
            ) * (1.0 / math.sqrt(width))
            labels = lax.broadcasted_iota(jnp.int32, logits.shape, 0)
            target = positive[c * held + level_of]
            picked = jnp.sum(jnp.where(labels == target, logits, 0.0), axis=0, keepdims=True)
            best = jnp.max(logits, axis=0, keepdims=True)
            total = jnp.sum(jnp.exp(logits - best), axis=0, keepdims=True)
            losses[level_of, c] = best + jnp.log(total) - picked
        for k in range(1, members):
            loss_copy(lax.rem(me + k, members), f, level_of).start()

    def drain(c, carry):
        for ph in range(CROSS):
            for o in range(dim_count):
                @pl.when((o <= d) & (d < dim_count - 1))
                def _():
                    right(ph, c, o).wait_send()

                @pl.when((o >= d) & (d > 0))
                def _():
                    left(ph, c, o).wait_send()

                pair(ph, c, o, f).wait_send()
        return carry

    lax.fori_loop(0, chunks, drain, 0)
    for k in range(3):
        for o in range(dim_count):
            @pl.when((o <= d) & (d < high))
            def _():
                chain_to(k, o, chain_right, to_right).wait_send()

            @pl.when((o >= d) & (d > low))
            def _():
                chain_to(k, o, chain_left, to_left).wait_send()

    @pl.when(active)
    def _():
        for k in range(3):
            both(k, f).wait_send()
        if split > 1:
            for k in range(1, split):
                t = lax.rem(b + k, split)
                plane(t, b).wait_send()
                plane_both(t, f).wait_send()
        for k in range(1, batch_count):
            cand_copy(lax.rem(b + k, batch_count), b).wait_send()
        for k in range(1, members):
            loss_copy(lax.rem(me + k, members), f, level_of).wait_send()

    for c in range(chunks):
        for level in range(held):
            @pl.when(jnp.logical_not(own_rows(c, level)))
            def _():
                row_copy(c, level).wait_send()

    for ff in range(field_count):
        for level in range(held):
            @pl.when(jnp.logical_not((f == ff) & (level_of == level)))
            def _():
                loss_copy(ff * dim_count + low + level, ff, level).wait_recv()

    for c in range(chunks):
        for level in range(held):
            loss_out[c * held + level] = losses[level, c]


def body(
    features, cross_weight, cross_bias, tower_weight, tower_bias, query_weight,
    user_vec, candidates, positive,
):
    counts = tuple(lax.axis_size(name) for name in ("batch", "field", "dim"))
    batch_count, field_count, dim_count = counts
    members = field_count * dim_count
    fl, el, row_count = features.shape
    columns = fl * el
    units, fields, width = tower_weight.shape
    low, held = tower_levels(dim_count)
    chunks = chunk_count(row_count, field_count, held)
    split = batch_count if units % (batch_count * 16) == 0 else 1
    part = units // split
    rc = row_count // chunks
    sub = rc // held
    run = chunks // field_count
    share = run * sub
    steps = (CROSS, chunks, dim_count)
    small = (3, dim_count)
    dma = pltpu.SemaphoreType.DMA
    vmem = pltpu.VMEM
    bf16 = jnp.bfloat16
    far = pl.BlockSpec(memory_space=pl.ANY)
    near = pl.BlockSpec(memory_space=pltpu.VMEM)
    crossed, losses = pl.pallas_call(
        functools.partial(rank_kernel, counts, (chunks, split)),
        out_shape=(
            jax.ShapeDtypeStruct(features.shape, bf16),
            jax.ShapeDtypeStruct((chunks * held, 1, sub), jnp.float32),
        ),
        in_specs=[far, far, near, far, far, far, near, far, near],
        out_specs=(near, near),
        scratch_shapes=[
            vmem((chunks, fields, width, rc), bf16),
            vmem((chunks, fields, width, rc), bf16),
            vmem((CROSS, fl, el, fields * width), bf16),
            vmem((chunks, held, fl, el, sub), bf16),
            vmem((fields, width, share), bf16),
            vmem((split, members, part, fields * width), bf16),
            vmem((members, 1, units), jnp.float32),
            vmem((split, members, part, share), jnp.float32),
            vmem((split, members, part, width), bf16),
            vmem((batch_count,) + candidates.shape, bf16),
            vmem((held, chunks, 1, sub), jnp.float32),
            dma((chunks,)), dma((CROSS, fields)), dma((fields,)), dma((3,)),
            dma(steps), dma(steps), dma(steps), dma(steps), dma(steps),
            dma((chunks, held)), dma((run, members)), dma(small), dma(small), dma(small),
            dma((3,)), dma((3,)),
            dma((split,)), dma((split,)), dma((split,)), dma((split,)),
            dma((batch_count,)), dma((batch_count,)), dma((members,)), dma((field_count, held)),
        ],
        compiler_params=pltpu.CompilerParams(
            collective_id=0, has_side_effects=True, vmem_limit_bytes=56 * 2**20),
        name="rank_forward",
    )(
        features,
        cross_weight.transpose(0, 1, 3, 2, 4),
        cross_bias.reshape(CROSS, columns, 1),
        tower_weight.transpose(1, 0, 2),
        tower_bias.reshape(1, units),
        query_weight.reshape(split, part, width),
        user_vec,
        candidates,
        positive.reshape(chunks * held, 1, sub),
    )
    return (crossed, losses.reshape(row_count))


def solution(mesh):
    placed = (
        P("field", "dim", "batch"),
        P(None, "field", "dim", None, None),
        P(None, "field", "dim"),
        P(("field", "dim"), None, None),
        P(("field", "dim")),
        P(("field", "dim"), None),
        P("batch", None),
        P("batch", None),
        P("batch"),
    )
    return jax.shard_map(
        body,
        mesh=mesh,
        in_specs=placed,
        out_specs=(P("field", "dim", "batch"), P("batch")),
        check_vma=False,
    )
```

```python
import functools
import math

import jax
import jax.numpy as jnp
from jax import lax
from jax.experimental import pallas as pl
from jax.experimental.pallas import tpu as pltpu
from jax.sharding import PartitionSpec as P

CROSS = 2
MESH = pl.DeviceIdType.MESH


def tower_levels(dim_count):
    held = min(2, dim_count)
    return (dim_count - held) // 2, held


def chunk_count(row_count, field_count, held):
    chunks = 2
    while chunks > field_count and row_count % (chunks * held * 128):
        chunks //= 2
    return chunks


def rank_kernel(
    counts, splits,
    feat, weight, bias, tower, tower_bias, query_weight, user, cand, positive,
    out, loss_out,
    x0, x1, flat, sent, rows, towers, biases, columns_bias, queries, cands, losses,
    feat_sem, weight_sem, tower_sem, small_sem,
    right_sem, left_sem, pair_sem, recv_sem, pair_recv,
    row_send, row_recv, chain_right, chain_left, chain_recv, both_send, both_recv,
    plane_send, plane_recv, plane_pair, plane_pair_recv,
    cand_send, cand_recv, loss_send, loss_recv,
):
    batch_count, field_count, dim_count = counts
    chunks, split = splits
    b = lax.axis_index("batch")
    f = lax.axis_index("field")
    d = lax.axis_index("dim")
    me = f * dim_count + d
    members = field_count * dim_count
    fl, el, row_count = feat.shape
    columns = fl * el
    fields, width, rc = x0.shape[1:]
    low, held = tower_levels(dim_count)
    high = low + held - 1
    level_of = d - low
    active = (d >= low) & (d <= high)
    sub = rc // held
    run = chunks // field_count
    share = run * sub
    part = towers.shape[2]
    units = split * part
    buffers = (x0, x1)
    other = field_count - 1 - f
    mine = b if split > 1 else 0
    to_right = jnp.minimum(d + 1, dim_count - 1)
    to_left = jnp.maximum(d - 1, 0)

    def remote(ref, send, recv, **where):
        return pltpu.make_async_remote_copy(
            ref, ref, send, recv, device_id=where, device_id_type=MESH)

    def place(ff, o):
        return pl.ds(ff * fl, fl), pl.ds(pl.multiple_of(o * el, el), el)

    def piece(ph, c, ff, o):
        fs, ds = place(ff, o)
        return buffers[ph].at[c, fs, ds, :]

    def right(ph, c, o):
        return remote(piece(ph, c, f, o), right_sem.at[ph, c, o], recv_sem.at[ph, c, o], dim=to_right)

    def left(ph, c, o):
        return remote(piece(ph, c, f, o), left_sem.at[ph, c, o], recv_sem.at[ph, c, o], dim=to_left)

    def pair(ph, c, o, ff):
        return remote(
            piece(ph, c, ff, o), pair_sem.at[ph, c, o], pair_recv.at[ph, c, o], field=other)

    def issue_own(ph, c):
        @pl.when(d < dim_count - 1)
        def _():
            right(ph, c, d).start()

        @pl.when(d > 0)
        def _():
            left(ph, c, d).start()

        pair(ph, c, d, f).start()

    def forwards(ph, c):
        for s in range(1, dim_count):
            @pl.when(d - s >= 0)
            def _():
                right(ph, c, d - s).wait_recv()

                @pl.when(d < dim_count - 1)
                def _():
                    right(ph, c, d - s).start()

                pair(ph, c, d - s, f).start()

            @pl.when(d + s < dim_count)
            def _():
                left(ph, c, d + s).wait_recv()

                @pl.when(d > 0)
                def _():
                    left(ph, c, d + s).start()

                pair(ph, c, d + s, f).start()
        for o in range(dim_count):
            pair(ph, c, o, other).wait_recv()

    def weight_copy(level, ff):
        return pltpu.make_async_copy(
            weight.at[level, :, ff],
            flat.at[level, :, :, pl.ds(pl.multiple_of(ff * width, width), width)],
            weight_sem.at[level, ff])

    def tower_copy(ff):
        return pltpu.make_async_copy(
            tower.at[ff, pl.ds(pl.multiple_of(mine * part, part), part), :],
            towers.at[mine, me, :, pl.ds(pl.multiple_of(ff * width, width), width)],
            tower_sem.at[ff])

    def each_field(act):
        def step(ff, carry):
            act(ff)
            return carry

        lax.fori_loop(0, fields, step, 0)

    small_refs = (
        lambda o: towers.at[mine, f * dim_count + o],
        lambda o: queries.at[:, f * dim_count + o],
        lambda o: biases.at[f * dim_count + o],
    )
    small_wide = (
        lambda ff: towers.at[mine, pl.ds(ff * dim_count, dim_count)],
        lambda ff: queries.at[:, pl.ds(ff * dim_count, dim_count)],
        lambda ff: biases.at[pl.ds(ff * dim_count, dim_count)],
    )

    def chain_to(k, o, sems, target):
        return remote(small_refs[k](o), sems.at[k, o], chain_recv.at[k, o], dim=target)

    def chain_own():
        for k in range(3):
            @pl.when(d < high)
            def _():
                chain_to(k, d, chain_right, to_right).start()

            @pl.when(d > low)
            def _():
                chain_to(k, d, chain_left, to_left).start()

    def chain_step(s):
        for k in range(3):
            @pl.when((d - s >= 0) & (d <= high))
            def _():
                chain_to(k, d - s, chain_right, to_right).wait_recv()

                @pl.when(d < high)
                def _():
                    chain_to(k, d - s, chain_right, to_right).start()

            @pl.when((d + s < dim_count) & (d >= low))
            def _():
                chain_to(k, d + s, chain_left, to_left).wait_recv()

                @pl.when(d > low)
                def _():
                    chain_to(k, d + s, chain_left, to_left).start()

    def both(k, ff):
        return remote(small_wide[k](ff), both_send.at[k], both_recv.at[k], field=other)

    def plane(t, source):
        return remote(
            towers.at[source, pl.ds(f * dim_count, dim_count)],
            plane_send.at[t], plane_recv.at[source], batch=t)

    def plane_both(source, ff):
        return remote(
            towers.at[source, pl.ds(ff * dim_count, dim_count)],
            plane_pair.at[source], plane_pair_recv.at[source], field=other)

    def cand_copy(t, source):
        return remote(cands.at[source], cand_send.at[t], cand_recv.at[source], batch=t)

    def loss_copy(m, ff, level):
        ref = losses.at[level, pl.ds(ff * run, run)]
        return remote(
            ref, loss_send.at[m], loss_recv.at[ff, level], field=m // dim_count, dim=m % dim_count)

    def row_copy(c, level):
        fs, ds = place(f, d)
        return pltpu.make_async_remote_copy(
            sent.at[c, level],
            rows.at[fs, ds, pl.ds(pl.multiple_of(lax.rem(c, run) * sub, sub), sub)],
            row_send.at[c, level], row_recv.at[lax.rem(c, run), me],
            device_id={"field": c // run, "dim": low + level}, device_id_type=MESH)

    def own_rows(c, level):
        return (c // run == f) & (level_of == level)

    def advance(ph, c):
        whole = buffers[ph][c].reshape(fields * width, rc)
        matrix = flat[ph].reshape(columns, fields * width)
        product = jnp.dot(matrix, whole, preferred_element_type=jnp.float32) + bias[ph]
        fs, ds = place(f, d)
        anchor = x0[c, fs, ds, :].astype(jnp.float32).reshape(columns, rc)
        current = buffers[ph][c, fs, ds, :].astype(jnp.float32).reshape(columns, rc)
        return (anchor * product + current).astype(jnp.bfloat16).reshape(fl, el, rc)

    own_copies = []
    for c in range(chunks):
        own_copies.append(pltpu.make_async_copy(
            feat.at[:, :, pl.ds(c * rc, rc)], piece(0, c, f, d), feat_sem.at[c]))
    small_copies = [
        pltpu.make_async_copy(query_weight, queries.at[:, me], small_sem.at[0]),
        pltpu.make_async_copy(tower_bias, biases.at[me], small_sem.at[1]),
        pltpu.make_async_copy(cand, cands.at[b], small_sem.at[2]),
    ]
    for copy in own_copies + small_copies:
        copy.start()
    each_field(lambda ff: tower_copy(ff).start())
    for level in range(CROSS):
        each_field(lambda ff: weight_copy(level, ff).start())

    barrier = pltpu.get_barrier_semaphore()
    for k in range(1, members):
        m = lax.rem(me + k, members)
        pl.semaphore_signal(
            barrier, inc=1, device_id={"field": m // dim_count, "dim": m % dim_count},
            device_id_type=MESH)
    for k in range(1, batch_count):
        pl.semaphore_signal(
            barrier, inc=1, device_id={"batch": lax.rem(b + k, batch_count)}, device_id_type=MESH)
    pl.semaphore_wait(barrier, members + batch_count - 2)
    for copy in own_copies:
        copy.wait()
    issue_own(0, 0)
    if chunks > 1:
        issue_own(0, 1)
    each_field(lambda ff: tower_copy(ff).wait())
    for copy in small_copies:
        copy.wait()
    chain_own()

    @pl.when(active)
    def _():
        for k in range(1, batch_count):
            cand_copy(lax.rem(b + k, batch_count), b).start()

    for level in range(CROSS):
        each_field(lambda ff: weight_copy(level, ff).wait())

    def first(c, carry):
        @pl.when(c + 2 < chunks)
        def _():
            issue_own(0, c + 2)

        forwards(0, c)
        fs, ds = place(f, d)
        x1[c, fs, ds, :] = advance(0, c)
        issue_own(1, c)

        for s in range(1, min(chunks, dim_count)):
            @pl.when(c == s)
            def _():
                chain_step(s)

        return carry

    lax.fori_loop(0, chunks, first, 0)
    for s in range(min(chunks, dim_count), dim_count):
        chain_step(s)

    @pl.when(active)
    def _():
        for k in range(3):
            both(k, f).start()
        if split > 1:
            for k in range(1, split):
                plane(lax.rem(b + k, split), b).start()

    def second(c, carry):
        forwards(1, c)
        new = advance(1, c)
        out[:, :, pl.ds(pl.multiple_of(c * rc, 128), rc)] = new
        for level in range(held):
            block = new[:, :, level * sub:(level + 1) * sub]

            @pl.when(own_rows(c, level))
            def _():
                fs, ds = place(f, d)
                rows[fs, ds, pl.ds(pl.multiple_of(lax.rem(c, run) * sub, sub), sub)] = block

            @pl.when(jnp.logical_not(own_rows(c, level)))
            def _():
                sent[c, level] = block
                row_copy(c, level).start()

        return carry

    lax.fori_loop(0, chunks, second, 0)

    def tower_block(s, query):
        matrix = towers[s].reshape(members * part, fields * width)
        pre = jnp.dot(
            matrix, rows[...].reshape(fields * width, share), preferred_element_type=jnp.float32)
        pre = pre + columns_bias[s].reshape(members * part, share)
        hidden = jnp.maximum(pre, 0.0).astype(jnp.bfloat16)
        return query + lax.dot_general(
            hidden, queries[s].reshape(members * part, width), (((0,), (0,)), ((), ())),
            preferred_element_type=jnp.float32)

    @pl.when(active)
    def _():
        if split > 1:
            for k in range(1, split):
                source = lax.rem(b + k, split)
                plane(source, source).wait_recv()
                plane_both(source, f).start()
        for k in range(3):
            both(k, other).wait_recv()
        for k in range(1, batch_count):
            source = lax.rem(b + k, batch_count)
            cand_copy(source, source).wait_recv()
        for m in range(members):
            block = jnp.broadcast_to(biases[m], (share, units)).T
            columns_bias[:, m] = block.reshape(split, part, share)
        if split > 1:
            for k in range(1, split):
                plane_both(lax.rem(b + k, split), other).wait_recv()
        for j in range(run):
            for k in range(1, members):
                m = lax.rem(me + k, members)
                fs, ds = place(m // dim_count, m % dim_count)
                remote(rows.at[fs, ds, pl.ds(j * sub, sub)], row_send.at[0, 0], row_recv.at[j, m],
                       field=m // dim_count, dim=m % dim_count).wait_recv()

        query = lax.fori_loop(0, split, tower_block, jnp.zeros((share, width), jnp.float32))
        all_cands = cands[...].reshape(-1, width)
        for j in range(run):
            c = f * run + j
            start = pl.multiple_of(c * rc + level_of * sub, sub)
            query_vec = (
                query[j * sub:(j + 1) * sub] + user[pl.ds(start, sub), :].astype(jnp.float32)
            ).astype(jnp.bfloat16)
            logits = lax.dot_general(
                all_cands, query_vec, (((1,), (1,)), ((), ())), preferred_element_type=jnp.float32
            ) * (1.0 / math.sqrt(width))
            labels = lax.broadcasted_iota(jnp.int32, logits.shape, 0)
            target = positive[c * held + level_of]
            picked = jnp.sum(jnp.where(labels == target, logits, 0.0), axis=0, keepdims=True)
            best = jnp.max(logits, axis=0, keepdims=True)
            total = jnp.sum(jnp.exp(logits - best), axis=0, keepdims=True)
            losses[level_of, c] = best + jnp.log(total) - picked
        for k in range(1, members):
            loss_copy(lax.rem(me + k, members), f, level_of).start()

    def drain(c, carry):
        for ph in range(CROSS):
            for o in range(dim_count):
                @pl.when((o <= d) & (d < dim_count - 1))
                def _():
                    right(ph, c, o).wait_send()

                @pl.when((o >= d) & (d > 0))
                def _():
                    left(ph, c, o).wait_send()

                pair(ph, c, o, f).wait_send()
        return carry

    lax.fori_loop(0, chunks, drain, 0)
    for k in range(3):
        for o in range(dim_count):
            @pl.when((o <= d) & (d < high))
            def _():
                chain_to(k, o, chain_right, to_right).wait_send()

            @pl.when((o >= d) & (d > low))
            def _():
                chain_to(k, o, chain_left, to_left).wait_send()

    @pl.when(active)
    def _():
        for k in range(3):
            both(k, f).wait_send()
        if split > 1:
            for k in range(1, split):
                t = lax.rem(b + k, split)
                plane(t, b).wait_send()
                plane_both(t, f).wait_send()
        for k in range(1, batch_count):
            cand_copy(lax.rem(b + k, batch_count), b).wait_send()
        for k in range(1, members):
            loss_copy(lax.rem(me + k, members), f, level_of).wait_send()

    for c in range(chunks):
        for level in range(held):
            @pl.when(jnp.logical_not(own_rows(c, level)))
            def _():
                row_copy(c, level).wait_send()

    for ff in range(field_count):
        for level in range(held):
            @pl.when(jnp.logical_not((f == ff) & (level_of == level)))
            def _():
                loss_copy(ff * dim_count + low + level, ff, level).wait_recv()

    for c in range(chunks):
        for level in range(held):
            loss_out[c * held + level] = losses[level, c]


def body(
    features, cross_weight, cross_bias, tower_weight, tower_bias, query_weight,
    user_vec, candidates, positive,
):
    counts = tuple(lax.axis_size(name) for name in ("batch", "field", "dim"))
    batch_count, field_count, dim_count = counts
    members = field_count * dim_count
    fl, el, row_count = features.shape
    columns = fl * el
    units, fields, width = tower_weight.shape
    low, held = tower_levels(dim_count)
    chunks = chunk_count(row_count, field_count, held)
    split = batch_count if units % (batch_count * 16) == 0 else 1
    part = units // split
    rc = row_count // chunks
    sub = rc // held
    run = chunks // field_count
    share = run * sub
    steps = (CROSS, chunks, dim_count)
    small = (3, dim_count)
    dma = pltpu.SemaphoreType.DMA
    vmem = pltpu.VMEM
    bf16 = jnp.bfloat16
    far = pl.BlockSpec(memory_space=pl.ANY)
    near = pl.BlockSpec(memory_space=pltpu.VMEM)
    crossed, losses = pl.pallas_call(
        functools.partial(rank_kernel, counts, (chunks, split)),
        out_shape=(
            jax.ShapeDtypeStruct(features.shape, bf16),
            jax.ShapeDtypeStruct((chunks * held, 1, sub), jnp.float32),
        ),
        in_specs=[far, far, near, far, far, far, near, far, near],
        out_specs=(near, near),
        scratch_shapes=[
            vmem((chunks, fields, width, rc), bf16),
            vmem((chunks, fields, width, rc), bf16),
            vmem((CROSS, fl, el, fields * width), bf16),
            vmem((chunks, held, fl, el, sub), bf16),
            vmem((fields, width, share), bf16),
            vmem((split, members, part, fields * width), bf16),
            vmem((members, 1, units), jnp.float32),
            vmem((split, members, part, share), jnp.float32),
            vmem((split, members, part, width), bf16),
            vmem((batch_count,) + candidates.shape, bf16),
            vmem((held, chunks, 1, sub), jnp.float32),
            dma((chunks,)), dma((CROSS, fields)), dma((fields,)), dma((3,)),
            dma(steps), dma(steps), dma(steps), dma(steps), dma(steps),
            dma((chunks, held)), dma((run, members)), dma(small), dma(small), dma(small),
            dma((3,)), dma((3,)),
            dma((split,)), dma((split,)), dma((split,)), dma((split,)),
            dma((batch_count,)), dma((batch_count,)), dma((members,)), dma((field_count, held)),
        ],
        compiler_params=pltpu.CompilerParams(
            collective_id=0, has_side_effects=True, vmem_limit_bytes=56 * 2**20),
        name="rank_forward",
    )(
        features,
        cross_weight.transpose(0, 1, 3, 2, 4),
        cross_bias.reshape(CROSS, columns, 1),
        tower_weight.transpose(1, 0, 2),
        tower_bias.reshape(1, units),
        query_weight.reshape(split, part, width),
        user_vec,
        candidates,
        positive.reshape(chunks * held, 1, sub),
    )
    return (crossed, losses.reshape(row_count))


def solution(mesh):
    placed = (
        P("field", "dim", "batch"),
        P(None, "field", "dim", None, None),
        P(None, "field", "dim"),
        P(("field", "dim"), None, None),
        P(("field", "dim")),
        P(("field", "dim"), None),
        P("batch", None),
        P("batch", None),
        P("batch"),
    )
    return jax.shard_map(
        body,
        mesh=mesh,
        in_specs=placed,
        out_specs=(P("field", "dim", "batch"), P("batch")),
        check_vma=False,
    )
```
